32 devices in a mesh: row: 4 (over y, x), col: 8 (over z, core).
Axes of the slice: x: 2, y: 2, z: 4, core: 2. Of those that a mesh axis runs over, the one named last changes fastest.
Arguments:
- features: bfloat16 [8192, 512], P(('row', 'col')), may hold values from -40 to 40
- w_query: bfloat16 [512, 512], replicated, may hold values from -0.25 to 0.25
- w_key: bfloat16 [512, 512], replicated, may hold values from -0.25 to 0.25
- w_value: bfloat16 [512, 512], replicated, may hold values from -0.25 to 0.25
- w_out: bfloat16 [512, 512], replicated, may hold values from -0.25 to 0.25
- pairs: int32 [4, 8, 128, 2], P('row', 'col'), may hold values from 0 to 15, as said below
- counts: int32 [4, 8], P('row', 'col'), may hold values from 16 to 128, as said below
- masks: int32 [4, 8, 128, 128, 4], P('row', 'col'), may hold values from -2147483648 to 2147483646, as said below
Outputs:
- updated: bfloat16 [8192, 512], P(('row', 'col'))
The draws below stay inside these ranges and needn't reach their ends.
Inputs may be any that keep to these rules, and one draw needn't show every extreme that they name: Within one device's list all 128 entries are distinct pairs; the first column is a query tile below 16, the second a key tile below 8. `counts`: some device has a full list of 128 entries in every draw. `masks`: any 32-bit pattern.
All inputs are finite; a program needn't handle non-finite values.
Results may differ from the reference program's by a relative error of at most 0.012.
The reference program's roundings to bfloat16 on the way count: a program that leaves them out, or rounds other values in their place, can miss the bound.
Values may be sent and summed in bfloat16 or wider, within the bound.
A program may use at most 128 MiB of HBM per device.

```python
import math
import jax
import jax.numpy as jnp
from jax import lax

D = 512
HEADS = 8
HEAD_DIM = 64
TILE = 128
MAXB = 128
NODE_DEV = 256
NODES = 8192
QTILES = 16
KTILES = 8
N_ROW = 4
N_COL = 8


def draw_features(key, part):
    base = jax.random.normal(key, (NODES, D), jnp.float32)
    return jnp.clip(base, -4.0, 4.0).astype(jnp.bfloat16)


def draw_pairs(key, part):
    keys = jax.random.split(jax.random.fold_in(key, 11), N_ROW * N_COL)
    ident = jax.vmap(lambda single: jax.random.permutation(single, QTILES * KTILES)[:MAXB])(keys)
    table = jnp.stack([ident // KTILES, ident % KTILES], -1).astype(jnp.int32)
    return table.reshape(N_ROW, N_COL, MAXB, 2)


def draw_counts(key, part):
    first = jax.random.randint(jax.random.fold_in(key, 1), (N_ROW * N_COL,), 0, MAXB)
    second = jax.random.randint(jax.random.fold_in(key, 2), (N_ROW * N_COL,), 0, MAXB)
    lowest = max(1, MAXB // 8)
    values = jnp.maximum(jnp.minimum(first, second) + 1, lowest)
    chosen = jax.random.randint(jax.random.fold_in(key, 3), (), 0, N_ROW * N_COL)
    values = jnp.where(jnp.arange(N_ROW * N_COL, dtype=jnp.int32) == chosen, MAXB, values)
    return values.astype(jnp.int32).reshape(N_ROW, N_COL)


def draw_masks(key, part):
    shape = (N_ROW, N_COL, MAXB, TILE, TILE // 32)
    return jax.random.randint(jax.random.fold_in(key, 5), shape, -2147483648, 2147483647, jnp.int32)


def noise(stream_key, extent, spread, bound, kind=jnp.bfloat16):
    return jnp.clip(spread * jax.random.normal(stream_key, extent, jnp.float32), -bound, bound).astype(kind)


def setup_inputs(seed: int = 0) -> dict:
    seeds = jax.random.split(jax.random.key(seed), 9)
    features = draw_features(jax.random.fold_in(seeds[8], 71), 0)
    w_query = noise(seeds[1], (D, D), D ** -0.5, 0.25)
    w_key = noise(seeds[2], (D, D), D ** -0.5, 0.25)
    w_value = noise(seeds[3], (D, D), D ** -0.5, 0.25)
    w_out = noise(seeds[4], (D, D), D ** -0.5, 0.25)
    pairs = draw_pairs(jax.random.fold_in(seeds[8], 71), 0)
    counts = draw_counts(jax.random.fold_in(seeds[8], 71), 0)
    masks = draw_masks(jax.random.fold_in(seeds[8], 71), 0)
    return dict(features=features, w_query=w_query, w_key=w_key, w_value=w_value, w_out=w_out, pairs=pairs, counts=counts, masks=masks)


def unpack_bits(words):
    shifts = jnp.broadcast_to(jnp.arange(32, dtype=jnp.int32), words.shape + (32,))
    bits = lax.shift_right_logical(words[..., None], shifts) & 1
    return bits.reshape(words.shape[:-1] + (words.shape[-1] * 32,)) == 1

def device_partial(q_part, k_part, v_part, my_pairs, my_count, my_words):
    scale = 1.0 / math.sqrt(HEAD_DIM)
    tiles_q = q_part.reshape(QTILES, TILE, HEADS, HEAD_DIM)
    tiles_k = k_part.reshape(KTILES, TILE, HEADS, HEAD_DIM)
    tiles_v = v_part.reshape(KTILES, TILE, HEADS, HEAD_DIM)
    qsel = my_pairs[:, 0]
    ksel = my_pairs[:, 1]
    q_blk = tiles_q[qsel].astype(jnp.float32)
    k_blk = tiles_k[ksel].astype(jnp.float32)
    v_blk = tiles_v[ksel].astype(jnp.float32)
    scores = jnp.einsum('gihd,gjhd->ghij', q_blk, k_blk) * scale
    valid = jnp.arange(MAXB, dtype=jnp.int32) < my_count
    live = unpack_bits(my_words) & valid[:, None, None]
    masked = jnp.where(live[:, None], scores, -jnp.inf)
    rowmax = masked.max(-1)
    tmax = jnp.zeros((QTILES, HEADS, TILE), jnp.float32).at[qsel].max(rowmax)
    prob = jnp.where(live[:, None], jnp.exp(scores - tmax[qsel][..., None]), 0.0).astype(jnp.bfloat16)
    probf = prob.astype(jnp.float32)
    den = jnp.exp(-tmax).at[qsel].add(probf.sum(-1))
    weighted = jnp.einsum('ghij,gjhd->gihd', probf, v_blk)
    num = jnp.zeros((QTILES, TILE, HEADS, HEAD_DIM), jnp.float32).at[qsel].add(weighted)
    return (tmax, num, den)

def reference(features, w_query, w_key, w_value, w_out, pairs, counts, masks):
    queries = jnp.dot(features, w_query, preferred_element_type=jnp.float32).astype(jnp.bfloat16)
    keys = jnp.dot(features, w_key, preferred_element_type=jnp.float32).astype(jnp.bfloat16)
    values = jnp.dot(features, w_value, preferred_element_type=jnp.float32).astype(jnp.bfloat16)
    q_rows = NODE_DEV * N_COL
    k_rows = NODE_DEV * N_ROW
    keys_grid = keys.reshape(N_ROW, N_COL, NODE_DEV, D)
    values_grid = values.reshape(N_ROW, N_COL, NODE_DEV, D)

    def per_row(r):
        q_part = lax.dynamic_slice_in_dim(queries, (r * q_rows).astype(jnp.int32), q_rows, 0)

        def per_col(c):
            k_part = lax.dynamic_index_in_dim(keys_grid, c, 1, keepdims=False).reshape(k_rows, D)
            v_part = lax.dynamic_index_in_dim(values_grid, c, 1, keepdims=False).reshape(k_rows, D)
            tmax, num, den = device_partial(q_part, k_part, v_part, pairs[r, c], counts[r, c], masks[r, c])
            part = (num / den.transpose(0, 2, 1)[..., None]).astype(jnp.bfloat16).astype(jnp.float32)
            return (tmax, part, den)
        tmax, part, den = lax.map(per_col, jnp.arange(N_COL, dtype=jnp.int32))
        top = tmax.max(0)
        weight = jnp.exp(tmax - top) * den
        total = weight.sum(0)
        numer = (part * weight.transpose(0, 1, 3, 2)[..., None]).sum(0)
        attended = (numer / total.transpose(0, 2, 1)[..., None]).astype(jnp.bfloat16).reshape(q_rows, D)
        return jnp.dot(attended, w_out, preferred_element_type=jnp.float32).astype(jnp.bfloat16)
    result = lax.map(per_row, jnp.arange(N_ROW, dtype=jnp.int32))
    return result.reshape(NODES, D)
```

```python
import functools
import math

import jax
import jax.numpy as jnp
from jax import lax
from jax.experimental import pallas as pl
from jax.experimental.pallas import tpu as pltpu
from jax.sharding import PartitionSpec as P

HEADS = 8
TILE = 128
BLOCK = 256
ONES = 16


def attend_group(
    group, table_ref, masks_ref, queries, k_ref, v_ref, part_ref, stat_ref, bias_ref, score_ref
):
    width, span = queries.shape
    keys = k_ref.shape[0]
    head = width // HEADS
    scale = 1.0 / math.sqrt(head)
    factor = scale * math.log2(math.e)
    k_tiles = keys // TILE
    tiles = span // TILE
    v_rows = v_ref.shape[0] // HEADS
    shift = 31 - lax.broadcasted_iota(jnp.int32, (32, TILE), 0)
    for b in range(k_tiles):
        for t in range(tiles):
            entry = table_ref[(group * tiles + t) * k_tiles + b]
            words = masks_ref[jnp.maximum(entry, 0)] * jnp.where(entry >= 0, 1, 0)
            for j in range(TILE // 32):
                bits = jnp.broadcast_to(words[j : j + 1, :], (32, TILE)) << shift
                bias_ref[pl.ds(b * TILE + j * 32, 32), pl.ds(t * TILE, TILE)] = jnp.where(
                    bits < 0, 0.0, -jnp.inf
                )
    step = min(BLOCK, keys)
    blocks = keys // step
    upper = lax.broadcasted_iota(jnp.int32, (2 * head, span), 0) < head

    def scores(h, block, top):
        pair = h // 2
        both = queries[pair * 2 * head : (pair + 1) * 2 * head, :]
        mine = jnp.where(upper == (h % 2 == 0), both, jnp.zeros_like(both))
        rows = slice(block * step, (block + 1) * step)
        raw = jnp.dot(
            k_ref[rows, pair * 2 * head : (pair + 1) * 2 * head],
            mine,
            preferred_element_type=jnp.float32,
        )
        raw = raw + bias_ref[rows, :]
        score_ref[h % 2, rows, :] = raw
        return jnp.maximum(top, jnp.max(raw.reshape(step // 8, 8, span), axis=0))

    def weighted(h, block, top, total):
        rows = slice(block * step, (block + 1) * step)
        prob = jnp.exp2((score_ref[h % 2, rows, :] - top) * factor).astype(jnp.bfloat16)
        term = jnp.dot(
            v_ref[h * v_rows : (h + 1) * v_rows, rows], prob, preferred_element_type=jnp.float32
        )
        return term if total is None else total + term

    def finish(h, top, total):
        peak = top * scale
        den = total[head : head + 1, :] + jnp.exp(-peak)
        part_ref[h * head : (h + 1) * head, :] = (total[:head, :] / den).astype(jnp.bfloat16)
        stat_ref[h : h + 1, :] = peak
        stat_ref[HEADS + h : HEADS + h + 1, :] = den

    zero = jnp.zeros((8, span), jnp.float32)
    tops = zero
    for block in range(blocks):
        tops = scores(0, block, tops)
    for h in range(HEADS):
        top = jnp.max(tops, axis=0, keepdims=True)
        total, tops = None, zero
        for block in range(blocks):
            if h + 1 < HEADS:
                tops = scores(h + 1, block, tops)
            total = weighted(h, block, top, total)
        finish(h, top, total)


def attention_kernel(table_ref, masks_ref, q_ref, k_ref, v_ref, part_ref, stat_ref, bias, score):
    attend_group(
        pl.program_id(0),
        table_ref,
        masks_ref,
        q_ref.at[0],
        k_ref,
        v_ref,
        part_ref.at[0],
        stat_ref.at[0],
        bias,
        score,
    )


def attention(table, masks, q_all, k_part, v_part):
    groups, width, span = q_all.shape
    keys = k_part.shape[0]
    whole = pl.BlockSpec(memory_space=pltpu.VMEM)
    return pl.pallas_call(
        attention_kernel,
        grid=(groups,),
        out_shape=(
            jax.ShapeDtypeStruct((groups, width, span), jnp.bfloat16),
            jax.ShapeDtypeStruct((groups, 2 * HEADS, span), jnp.float32),
        ),
        in_specs=[
            pl.BlockSpec(memory_space=pltpu.SMEM),
            whole,
            pl.BlockSpec((1, width, span), lambda g: (g, 0, 0)),
            whole,
            whole,
        ],
        out_specs=(
            pl.BlockSpec((1, width, span), lambda g: (g, 0, 0)),
            pl.BlockSpec((1, 2 * HEADS, span), lambda g: (g, 0, 0)),
        ),
        scratch_shapes=[
            pltpu.VMEM((keys, span), jnp.float32),
            pltpu.VMEM((2, keys, span), jnp.float32),
        ],
        compiler_params=pltpu.CompilerParams(
            dimension_semantics=("arbitrary",), vmem_limit_bytes=48 * 1024 * 1024
        ),
        name="attention",
    )(table, masks, q_all, k_part, v_part)


def entry_table(pairs, count, q_tiles, k_tiles):
    entries = pairs.shape[0]
    ids = lax.broadcasted_iota(jnp.int32, (q_tiles * k_tiles, entries), 1)
    cell = lax.broadcasted_iota(jnp.int32, (q_tiles * k_tiles, entries), 0)
    code = (pairs[:, 0] * k_tiles + pairs[:, 1])[None, :]
    return jnp.max(jnp.where((code == cell) & (ids < count), ids, -1), axis=1)


def body(features, w_query, w_key, w_value, w_out, pairs, counts, masks):
    nodes, width = features.shape
    head = width // HEADS
    f32 = jnp.float32
    gathered = lax.all_gather(features, "row", axis=0, tiled=True)
    q_local = lax.dot_general(
        w_query, features, (((0,), (1,)), ((), ())), preferred_element_type=f32
    ).astype(jnp.bfloat16)
    q_all = lax.all_gather(q_local, "col", axis=0)
    k_part = jnp.dot(gathered, w_key, preferred_element_type=f32).astype(jnp.bfloat16)
    v_part = lax.dot_general(
        w_value, gathered, (((0,), (1,)), ((), ())), preferred_element_type=f32
    ).astype(jnp.bfloat16)
    keys = k_part.shape[0]
    v_part = jnp.concatenate(
        [v_part.reshape(HEADS, head, keys), jnp.ones((HEADS, ONES, keys), jnp.bfloat16)], axis=1
    ).reshape(HEADS * (head + ONES), keys)
    groups = q_all.shape[0]
    table = entry_table(pairs[0, 0], counts[0, 0], groups * nodes // TILE, keys // TILE)
    words = masks[0, 0].transpose(0, 2, 1)
    part, stat = attention(table, words, q_all, k_part, v_part)
    part = lax.all_to_all(part, "col", 0, 0)
    stat = lax.all_to_all(stat, "col", 0, 0)
    peak, den = stat[:, :HEADS], stat[:, HEADS:]
    top = jnp.max(peak, axis=0)
    weight = jnp.exp(peak - top) * den
    total = weight.sum(0)
    numer = (part.reshape(groups, HEADS, head, nodes).astype(f32) * weight[:, :, None, :]).sum(0)
    attended = (numer / total[:, None, :]).astype(jnp.bfloat16).reshape(width, nodes)
    return lax.dot_general(
        attended, w_out, (((0,), (0,)), ((), ())), preferred_element_type=f32
    ).astype(jnp.bfloat16)


def solution(mesh):
    in_specs = (
        P(("row", "col"), None),
        P(),
        P(),
        P(),
        P(),
        P("row", "col", None, None),
        P("row", "col"),
        P("row", "col", None, None, None),
    )
    out_specs = P(("row", "col"), None)
    return jax.shard_map(body, mesh=mesh, in_specs=in_specs, out_specs=out_specs, check_vma=False)
```

```python
import functools
import math

import jax
import jax.numpy as jnp
from jax import lax
from jax.experimental import pallas as pl
from jax.experimental.pallas import tpu as pltpu
from jax.sharding import PartitionSpec as P

HEADS = 8
TILE = 128
BLOCK = 256
ONES = 16


def attend_group(
    group, table_ref, masks_ref, queries, k_ref, v_ref, part_ref, stat_ref, bias_ref, score_ref
):
    width, span = queries.shape
    keys = k_ref.shape[0]
    head = width // HEADS
    scale = 1.0 / math.sqrt(head)
    factor = scale * math.log2(math.e)
    k_tiles = keys // TILE
    tiles = span // TILE
    v_rows = v_ref.shape[0] // HEADS
    shift = 31 - lax.broadcasted_iota(jnp.int32, (32, TILE), 0)
    for b in range(k_tiles):
        for t in range(tiles):
            entry = table_ref[(group * tiles + t) * k_tiles + b]
            words = masks_ref[jnp.maximum(entry, 0)] * jnp.where(entry >= 0, 1, 0)
            for j in range(TILE // 32):
                bits = jnp.broadcast_to(words[j : j + 1, :], (32, TILE)) << shift
                bias_ref[pl.ds(b * TILE + j * 32, 32), pl.ds(t * TILE, TILE)] = jnp.where(
                    bits < 0, 0.0, -jnp.inf
                )
    step = min(BLOCK, keys)
    blocks = keys // step
    upper = lax.broadcasted_iota(jnp.int32, (2 * head, span), 0) < head

    def scores(h, block, top):
        pair = h // 2
        both = queries[pair * 2 * head : (pair + 1) * 2 * head, :]
        mine = jnp.where(upper == (h % 2 == 0), both, jnp.zeros_like(both))
        rows = slice(block * step, (block + 1) * step)
        raw = jnp.dot(
            k_ref[rows, pair * 2 * head : (pair + 1) * 2 * head],
            mine,
            preferred_element_type=jnp.float32,
        )
        raw = raw + bias_ref[rows, :]
        score_ref[h % 2, rows, :] = raw
        return jnp.maximum(top, jnp.max(raw.reshape(step // 8, 8, span), axis=0))

    def weighted(h, block, top, total):
        rows = slice(block * step, (block + 1) * step)
        prob = jnp.exp2((score_ref[h % 2, rows, :] - top) * factor).astype(jnp.bfloat16)
        term = jnp.dot(
            v_ref[h * v_rows : (h + 1) * v_rows, rows], prob, preferred_element_type=jnp.float32
        )
        return term if total is None else total + term

    def finish(h, top, total):
        peak = top * scale
        den = total[head : head + 1, :] + jnp.exp(-peak)
        part_ref[h * head : (h + 1) * head, :] = (total[:head, :] / den).astype(jnp.bfloat16)
        stat_ref[h : h + 1, :] = peak
        stat_ref[HEADS + h : HEADS + h + 1, :] = den

    zero = jnp.zeros((8, span), jnp.float32)
    tops = zero
    for block in range(blocks):
        tops = scores(0, block, tops)
    for h in range(HEADS):
        top = jnp.max(tops, axis=0, keepdims=True)
        total, tops = None, zero
        for block in range(blocks):
            if h + 1 < HEADS:
                tops = scores(h + 1, block, tops)
            total = weighted(h, block, top, total)
        finish(h, top, total)


MESH = pl.DeviceIdType.MESH


def fused_kernel(
    rows,
    cols,
    table_ref,
    masks_ref,
    features_ref,
    wq_ref,
    wk_ref,
    wv_ref,
    wo_ref,
    out_ref,
    frow,
    fcol,
    wq_t,
    wv_t,
    k_all,
    v_all,
    q_now,
    part,
    stat,
    pair_part,
    pair_stat,
    both_part,
    both_stat,
    fin_part,
    fin_stat,
    bias,
    score,
    row_send,
    row_recv,
    col_recv,
    right_send,
    left_send,
    share_left,
    share_right,
    pair_send,
    pair_recv,
    fin_send,
    fin_recv,
):
    nodes, width = features_ref.shape
    head = width // HEADS
    f32 = jnp.float32
    chips = cols // 2
    r, c = lax.axis_index("row"), lax.axis_index("col")
    m, k = c // 2, lax.rem(c, 2)
    mate = (r, m * 2 + 1 - k)

    def at(chip):
        return (r, chip * 2 + k)

    def send(src, dst, send_sem, recv_sem, device):
        return pltpu.make_async_remote_copy(
            src_ref=src,
            dst_ref=dst,
            send_sem=send_sem,
            recv_sem=recv_sem,
            device_id=device,
            device_id_type=MESH,
        )

    barrier = pltpu.get_barrier_semaphore()
    pl.semaphore_signal(barrier, inc=1, device_id=mate, device_id_type=MESH)
    for d in range(1, rows):
        peer = (lax.rem(r + d, rows), c)
        pl.semaphore_signal(barrier, inc=1, device_id=peer, device_id_type=MESH)
    for d in range(1, chips):
        peer = at(lax.rem(m + d, chips))
        pl.semaphore_signal(barrier, inc=1, device_id=peer, device_id_type=MESH)
    pl.semaphore_wait(barrier, 1 + rows - 1 + chips - 1)

    has_right, has_left = m + 1 < chips, m >= 1

    def to_right(s):
        slot = (m - s) * 2 + k
        src = features_ref if s == 0 else fcol.at[slot]
        return send(src, fcol.at[slot], right_send.at[s], col_recv.at[slot], at(m + 1))

    def to_left(s):
        slot = (m + s) * 2 + k
        src = features_ref if s == 0 else fcol.at[slot]
        return send(src, fcol.at[slot], left_send.at[s], col_recv.at[slot], at(m - 1))

    def to_mate_left(s):
        slot = (m - s) * 2 + k
        src = features_ref if s == 0 else fcol.at[slot]
        return send(src, fcol.at[slot], share_left.at[s], col_recv.at[slot], mate)

    def to_mate_right(s):
        slot = (m + s) * 2 + k
        return send(fcol.at[slot], fcol.at[slot], share_right.at[s], col_recv.at[slot], mate)

    def to_row(d):
        return send(
            features_ref, frow.at[r], row_send.at[d], row_recv.at[r], (lax.rem(r + d, rows), c)
        )

    def await_col(slot):
        send(fcol.at[slot], fcol.at[slot], right_send.at[0], col_recv.at[slot], mate).wait_recv()

    @pl.when(has_right)
    def _():
        to_right(0).start()

    @pl.when(has_left)
    def _():
        to_left(0).start()

    for d in range(1, rows):
        to_row(d).start()
    to_mate_left(0).start()

    frow[r] = features_ref[...]
    fcol[c] = features_ref[...]
    wq_t[...] = wq_ref[...].T
    wv_t[...] = wv_ref[...].T
    for h in range(HEADS):
        v_all[h * (head + ONES) + head : (h + 1) * (head + ONES), :] = jnp.ones(
            (ONES, rows * nodes), jnp.bfloat16
        )

    def project_row(slot):
        block = frow[slot]
        lane = pl.ds(pl.multiple_of(slot * nodes, nodes), nodes)
        k_all[lane, :] = jnp.dot(block, wk_ref[...], preferred_element_type=f32).astype(
            jnp.bfloat16
        )
        value = lax.dot_general(
            wv_t[...], block, (((1,), (1,)), ((), ())), preferred_element_type=f32
        ).astype(jnp.bfloat16)
        for h in range(HEADS):
            v_all[h * (head + ONES) : h * (head + ONES) + head, lane] = value[
                h * head : (h + 1) * head, :
            ]

    project_row(r)
    for s in range(1, chips):
        if s == chips - 1:
            for d in range(1, rows):
                slot = lax.rem(r + rows - d, rows)
                send(
                    frow.at[slot], frow.at[slot], row_send.at[0], row_recv.at[slot], mate
                ).wait_recv()
                project_row(slot)

        @pl.when(m >= s)
        def _():
            await_col((m - s) * 2 + k)
            to_mate_left(s).start()
            if s + 1 < chips:

                @pl.when(has_right)
                def _():
                    to_right(s).start()

        @pl.when(m + s < chips)
        def _():
            await_col((m + s) * 2 + k)
            to_mate_right(s).start()
            if s + 1 < chips:

                @pl.when(has_left)
                def _():
                    to_left(s).start()

    def pair_copies(i, j):
        return (
            send(part.at[i], pair_part.at[j], pair_send.at[j, 0], pair_recv.at[j, 0], mate),
            send(stat.at[i], pair_stat.at[j], pair_send.at[j, 1], pair_recv.at[j, 1], mate),
        )

    def fin_copies(j):
        owner = at(lax.rem(m + 1 + j, chips))
        return (
            send(both_part.at[j], fin_part.at[j], fin_send.at[j, 0], fin_recv.at[j, 0], owner),
            send(both_stat.at[j], fin_stat.at[j], fin_send.at[j, 1], fin_recv.at[j, 1], owner),
        )

    def weigh(sources):
        peaks = [ref[0:HEADS, :] for _, ref in sources]
        top = functools.reduce(jnp.maximum, peaks)
        weights = [
            jnp.exp(peak - top) * ref[HEADS : 2 * HEADS, :]
            for peak, (_, ref) in zip(peaks, sources)
        ]
        total = functools.reduce(jnp.add, weights)
        return top, weights, total

    def blend(sources, weights, total, h):
        rows_of = slice(h * head, (h + 1) * head)
        numer = functools.reduce(
            jnp.add,
            [
                ref[rows_of, :].astype(f32) * weight[h : h + 1, :]
                for weight, (ref, _) in zip(weights, sources)
            ],
        )
        return (numer / total[h : h + 1, :]).astype(jnp.bfloat16)

    def merge(j):
        for copy in pair_copies(0, j):
            copy.wait_recv()
        mine = 2 * j + k
        sources = [(part.at[mine], stat.at[mine]), (pair_part.at[j], pair_stat.at[j])]
        top, weights, total = weigh(sources)
        both_stat[j, 0:HEADS, :] = top
        both_stat[j, HEADS : 2 * HEADS, :] = total
        for h in range(HEADS):
            both_part[j, h * head : (h + 1) * head, :] = blend(sources, weights, total, h)
        for copy in fin_copies(j):
            copy.start()

    def turn(i, carry):
        j = i // 2
        odd = lax.rem(i, 2)
        chip = lax.rem(m + 1 + j, chips)
        group = chip * 2 + odd

        @pl.when(odd != k)
        def _():
            await_col(group)

        q_now[...] = lax.dot_general(
            wq_t[...], fcol[group], (((1,), (1,)), ((), ())), preferred_element_type=f32
        ).astype(jnp.bfloat16)
        attend_group(
            group,
            table_ref,
            masks_ref,
            q_now,
            k_all,
            v_all,
            part.at[i],
            stat.at[i],
            bias,
            score,
        )

        @pl.when(odd != k)
        def _():
            for copy in pair_copies(i, j):
                copy.start()

        @pl.when((odd == 0) & (i > 0))
        def _():
            merge(j - 1)

        return carry

    lax.fori_loop(0, cols, turn, 0)

    last = chips - 1
    mine = 2 * last + k
    for copy in pair_copies(0, last):
        copy.wait_recv()
    for j in range(last):
        for copy in fin_copies(j):
            copy.wait_recv()
    sources = [(part.at[mine], stat.at[mine]), (pair_part.at[last], pair_stat.at[last])]
    sources += [(fin_part.at[j], fin_stat.at[j]) for j in range(last)]
    _, weights, total = weigh(sources)
    for h in range(HEADS):
        q_now[h * head : (h + 1) * head, :] = blend(sources, weights, total, h)
    out_ref[...] = lax.dot_general(
        q_now[...], wo_ref[...], (((0,), (0,)), ((), ())), preferred_element_type=f32
    ).astype(jnp.bfloat16)

    for d in range(1, rows):
        to_row(d).wait_send()
    to_mate_left(0).wait_send()
    for s in range(chips):

        @pl.when(m >= s)
        def _():
            if s > 0:
                to_mate_left(s).wait_send()
            if s + 1 < chips:

                @pl.when(has_right)
                def _():
                    to_right(s).wait_send()

        @pl.when(m + s < chips)
        def _():
            if s > 0:
                to_mate_right(s).wait_send()
            if s + 1 < chips:

                @pl.when(has_left)
                def _():
                    to_left(s).wait_send()

    for j in range(chips):
        for copy in pair_copies(0, j):
            copy.wait_send()
    for j in range(last):
        for copy in fin_copies(j):
            copy.wait_send()


def fused(mesh_shape, table, masks, features, w_query, w_key, w_value, w_out):
    rows, cols = mesh_shape["row"], mesh_shape["col"]
    chips = cols // 2
    nodes, width = features.shape
    keys = rows * nodes
    head = width // HEADS
    bf16, f32 = jnp.bfloat16, jnp.float32
    whole = pl.BlockSpec(memory_space=pltpu.VMEM)
    dma = pltpu.SemaphoreType.DMA
    return pl.pallas_call(
        functools.partial(fused_kernel, rows, cols),
        out_shape=jax.ShapeDtypeStruct((nodes, width), bf16),
        in_specs=[pl.BlockSpec(memory_space=pltpu.SMEM)] + [whole] * 6,
        out_specs=whole,
        scratch_shapes=[
            pltpu.VMEM((rows, nodes, width), bf16),
            pltpu.VMEM((cols, nodes, width), bf16),
            pltpu.VMEM((width, width), bf16),
            pltpu.VMEM((width, width), bf16),
            pltpu.VMEM((keys, width), bf16),
            pltpu.VMEM((HEADS * (head + ONES), keys), bf16),
            pltpu.VMEM((width, nodes), bf16),
            pltpu.VMEM((cols, width, nodes), bf16),
            pltpu.VMEM((cols, 2 * HEADS, nodes), f32),
            pltpu.VMEM((chips, width, nodes), bf16),
            pltpu.VMEM((chips, 2 * HEADS, nodes), f32),
            pltpu.VMEM((chips, width, nodes), bf16),
            pltpu.VMEM((chips, 2 * HEADS, nodes), f32),
            pltpu.VMEM((chips, width, nodes), bf16),
            pltpu.VMEM((chips, 2 * HEADS, nodes), f32),
            pltpu.VMEM((keys, nodes), f32),
            pltpu.VMEM((2, keys, nodes), f32),
            dma((rows,)),
            dma((rows,)),
            dma((cols,)),
            dma((chips,)),
            dma((chips,)),
            dma((chips,)),
            dma((chips,)),
            dma((chips, 2)),
            dma((chips, 2)),
            dma((chips, 2)),
            dma((chips, 2)),
        ],
        compiler_params=pltpu.CompilerParams(
            collective_id=0, has_side_effects=True, vmem_limit_bytes=60 * 1024 * 1024
        ),
        name="fused",
    )(table, masks, features, w_query, w_key, w_value, w_out)


def entry_table(pairs, count, q_tiles, k_tiles):
    entries = pairs.shape[0]
    ids = lax.broadcasted_iota(jnp.int32, (q_tiles * k_tiles, entries), 1)
    cell = lax.broadcasted_iota(jnp.int32, (q_tiles * k_tiles, entries), 0)
    code = (pairs[:, 0] * k_tiles + pairs[:, 1])[None, :]
    return jnp.max(jnp.where((code == cell) & (ids < count), ids, -1), axis=1)


def body(mesh_shape, features, w_query, w_key, w_value, w_out, pairs, counts, masks):
    nodes = features.shape[0]
    rows, cols = mesh_shape["row"], mesh_shape["col"]
    table = entry_table(pairs[0, 0], counts[0, 0], cols * nodes // TILE, rows * nodes // TILE)
    words = masks[0, 0].transpose(0, 2, 1)
    return fused(mesh_shape, table, words, features, w_query, w_key, w_value, w_out)


def solution(mesh):
    in_specs = (
        P(("row", "col"), None),
        P(),
        P(),
        P(),
        P(),
        P("row", "col", None, None),
        P("row", "col"),
        P("row", "col", None, None, None),
    )
    out_specs = P(("row", "col"), None)
    return jax.shard_map(
        functools.partial(body, dict(mesh.shape)), mesh=mesh, in_specs=in_specs, out_specs=out_specs, check_vma=False)
```

```python
import functools
import math

import jax
import jax.numpy as jnp
from jax import lax
from jax.experimental import pallas as pl
from jax.experimental.pallas import tpu as pltpu
from jax.sharding import PartitionSpec as P

HEADS = 8
TILE = 128
BLOCK = 256
ONES = 16


def build_bias(group, table_ref, masks_ref, bias_ref):
    keys, span = bias_ref.shape
    k_tiles = keys // TILE
    tiles = span // TILE
    shift = 31 - lax.broadcasted_iota(jnp.int32, (32, TILE), 0)
    for b in range(k_tiles):
        for t in range(tiles):
            entry = table_ref[(group * tiles + t) * k_tiles + b]
            words = masks_ref[jnp.maximum(entry, 0)] * jnp.where(entry >= 0, 1, 0)
            for j in range(TILE // 32):
                bits = jnp.broadcast_to(words[j : j + 1, :], (32, TILE)) << shift
                bias_ref[pl.ds(b * TILE + j * 32, 32), pl.ds(t * TILE, TILE)] = jnp.where(
                    bits < 0, 0.0, -jnp.inf
                )


def attend_group(queries, k_ref, v_ref, part_ref, stat_ref, bias_ref, score_ref):
    width, span = queries.shape
    keys = k_ref.shape[0]
    head = width // HEADS
    scale = 1.0 / math.sqrt(head)
    factor = scale * math.log2(math.e)
    v_rows = v_ref.shape[0] // HEADS
    step = min(BLOCK, keys)
    blocks = keys // step
    upper = lax.broadcasted_iota(jnp.int32, (2 * head, span), 0) < head

    def scores(h, block, top):
        pair = h // 2
        both = queries[pair * 2 * head : (pair + 1) * 2 * head, :]
        mine = jnp.where(upper == (h % 2 == 0), both, jnp.zeros_like(both))
        rows = slice(block * step, (block + 1) * step)
        raw = jnp.dot(
            k_ref[rows, pair * 2 * head : (pair + 1) * 2 * head],
            mine,
            preferred_element_type=jnp.float32,
        )
        raw = raw + bias_ref[rows, :]
        score_ref[h % 2, rows, :] = raw
        return jnp.maximum(top, jnp.max(raw.reshape(step // 8, 8, span), axis=0))

    def weighted(h, block, top, total):
        rows = slice(block * step, (block + 1) * step)
        prob = jnp.exp2((score_ref[h % 2, rows, :] - top) * factor).astype(jnp.bfloat16)
        term = jnp.dot(
            v_ref[h * v_rows : (h + 1) * v_rows, rows], prob, preferred_element_type=jnp.float32
        )
        return term if total is None else total + term

    def finish(h, top, total):
        peak = top * scale
        den = total[head : head + 1, :] + jnp.exp(-peak)
        part_ref[h * head : (h + 1) * head, :] = (total[:head, :] / den).astype(jnp.bfloat16)
        stat_ref[h : h + 1, :] = peak
        stat_ref[HEADS + h : HEADS + h + 1, :] = den

    zero = jnp.zeros((8, span), jnp.float32)
    tops = zero
    for block in range(blocks):
        tops = scores(0, block, tops)
    for h in range(HEADS):
        top = jnp.max(tops, axis=0, keepdims=True)
        total, tops = None, zero
        for block in range(blocks):
            if h + 1 < HEADS:
                tops = scores(h + 1, block, tops)
            total = weighted(h, block, top, total)
        finish(h, top, total)


MESH = pl.DeviceIdType.MESH


def fused_kernel(
    rows,
    cols,
    table_ref,
    masks_ref,
    features_ref,
    wq_ref,
    wk_ref,
    wv_ref,
    out_ref,
    frow,
    fcol,
    wq_t,
    wv_t,
    k_all,
    v_all,
    q_now,
    part,
    stat,
    pair_part,
    pair_stat,
    both_part,
    both_stat,
    fin_part,
    fin_stat,
    bias,
    score,
    row_send,
    row_recv,
    col_recv,
    right_send,
    left_send,
    share_left,
    share_right,
    pair_send,
    pair_recv,
    fin_send,
    fin_recv,
):
    nodes, width = features_ref.shape
    head = width // HEADS
    f32 = jnp.float32
    chips = cols // 2
    r, c = lax.axis_index("row"), lax.axis_index("col")
    m, k = c // 2, lax.rem(c, 2)
    mate = (r, m * 2 + 1 - k)

    half = chips // 2

    def at(chip):
        return (r, chip * 2 + k)

    def owner_chip(j):
        return lax.rem(m + jnp.where(j == 0, half, jnp.where(j < half, j, j + 1)), chips)

    def flip(place, b):
        return place + 1 - 2 * lax.rem(place, 2) if b else place

    def row_to(d):
        if rows % 2:
            return lax.rem(r + d, rows)
        return flip(lax.rem(r + d // 2 * 2, rows), d % 2)

    def row_from(d):
        if rows % 2:
            return lax.rem(r + rows - d, rows)
        return lax.rem(flip(r, d % 2) + rows - d // 2 * 2, rows)

    def send(src, dst, send_sem, recv_sem, device):
        return pltpu.make_async_remote_copy(
            src_ref=src,
            dst_ref=dst,
            send_sem=send_sem,
            recv_sem=recv_sem,
            device_id=device,
            device_id_type=MESH,
        )

    barrier = pltpu.get_barrier_semaphore()
    pl.semaphore_signal(barrier, inc=1, device_id=mate, device_id_type=MESH)
    for d in range(1, rows):
        peer = (lax.rem(r + d, rows), c)
        pl.semaphore_signal(barrier, inc=1, device_id=peer, device_id_type=MESH)
    for d in range(1, chips):
        peer = at(lax.rem(m + d, chips))
        pl.semaphore_signal(barrier, inc=1, device_id=peer, device_id_type=MESH)
    pl.semaphore_wait(barrier, 1 + rows - 1 + chips - 1)

    has_right, has_left = m + 1 < chips, m >= 1

    def to_right(s):
        slot = (m - s) * 2 + k
        src = features_ref if s == 0 else fcol.at[slot]
        return send(src, fcol.at[slot], right_send.at[s], col_recv.at[slot], at(m + 1))

    def to_left(s):
        slot = (m + s) * 2 + k
        src = features_ref if s == 0 else fcol.at[slot]
        return send(src, fcol.at[slot], left_send.at[s], col_recv.at[slot], at(m - 1))

    def to_mate_left(s):
        slot = (m - s) * 2 + k
        src = features_ref if s == 0 else fcol.at[slot]
        return send(src, fcol.at[slot], share_left.at[s], col_recv.at[slot], mate)

    def to_mate_right(s):
        slot = (m + s) * 2 + k
        return send(fcol.at[slot], fcol.at[slot], share_right.at[s], col_recv.at[slot], mate)

    def to_row(d):
        return send(
            features_ref, frow.at[r], row_send.at[d], row_recv.at[r], (row_to(d), c)
        )

    def await_col(slot):
        send(fcol.at[slot], fcol.at[slot], right_send.at[0], col_recv.at[slot], mate).wait_recv()

    @pl.when(has_right)
    def _():
        to_right(0).start()

    @pl.when(has_left)
    def _():
        to_left(0).start()

    for d in range(1, rows):
        to_row(d).start()
    to_mate_left(0).start()

    frow[r] = features_ref[...]
    fcol[c] = features_ref[...]
    wq_t[...] = wq_ref[...].T
    wv_t[...] = wv_ref[...].T
    for h in range(HEADS):
        v_all[h * (head + ONES) + head : (h + 1) * (head + ONES), :] = jnp.ones(
            (ONES, rows * nodes), jnp.bfloat16
        )

    def project_row(slot):
        block = frow[slot]
        lane = pl.ds(pl.multiple_of(slot * nodes, nodes), nodes)
        k_all[lane, :] = jnp.dot(block, wk_ref[...], preferred_element_type=f32).astype(
            jnp.bfloat16
        )
        value = lax.dot_general(
            wv_t[...], block, (((1,), (1,)), ((), ())), preferred_element_type=f32
        ).astype(jnp.bfloat16)
        for h in range(HEADS):
            v_all[h * (head + ONES) : h * (head + ONES) + head, lane] = value[
                h * head : (h + 1) * head, :
            ]

    project_row(r)

    def await_row(d):
        slot = row_from(d)
        send(frow.at[slot], frow.at[slot], row_send.at[0], row_recv.at[slot], mate).wait_recv()
        project_row(slot)

    def relay(s):
        @pl.when(m >= s)
        def _():
            await_col((m - s) * 2 + k)
            to_mate_left(s).start()
            if s + 1 < chips:

                @pl.when(has_right)
                def _():
                    to_right(s).start()

        @pl.when(m + s < chips)
        def _():
            await_col((m + s) * 2 + k)
            to_mate_right(s).start()
            if s + 1 < chips:

                @pl.when(has_left)
                def _():
                    to_left(s).start()

    late = min(chips - half + 1, chips)
    for s in range(1, late):
        relay(s)
        if s == 1:
            for d in range(1, rows - 1):
                await_row(d)
    for d in range(rows - 1 if chips > 1 and late > 1 else 1, rows):
        await_row(d)

    def pair_copies(i, j):
        return (
            send(part.at[i], pair_part.at[j], pair_send.at[j, 0], pair_recv.at[j, 0], mate),
            send(stat.at[i], pair_stat.at[j], pair_send.at[j, 1], pair_recv.at[j, 1], mate),
        )

    def fin_copies(j):
        owner = at(owner_chip(j))
        return (
            send(both_part.at[j], fin_part.at[j], fin_send.at[j, 0], fin_recv.at[j, 0], owner),
            send(both_stat.at[j], fin_stat.at[j], fin_send.at[j, 1], fin_recv.at[j, 1], owner),
        )

    def weigh(sources):
        peaks = [ref[0:HEADS, :] for _, ref in sources]
        top = functools.reduce(jnp.maximum, peaks)
        weights = [
            jnp.exp(peak - top) * ref[HEADS : 2 * HEADS, :]
            for peak, (_, ref) in zip(peaks, sources)
        ]
        total = functools.reduce(jnp.add, weights)
        return top, weights, total

    def blend(sources, weights, total, h):
        rows_of = slice(h * head, (h + 1) * head)
        numer = functools.reduce(
            jnp.add,
            [
                ref[rows_of, :].astype(f32) * weight[h : h + 1, :]
                for weight, (ref, _) in zip(weights, sources)
            ],
        )
        return (numer / total[h : h + 1, :]).astype(jnp.bfloat16)

    def merge(j):
        for copy in pair_copies(0, j):
            copy.wait_recv()
        mine = 2 * j + k
        sources = [(part.at[mine], stat.at[mine]), (pair_part.at[j], pair_stat.at[j])]
        top, weights, total = weigh(sources)
        both_stat[j, 0:HEADS, :] = top
        both_stat[j, HEADS : 2 * HEADS, :] = total
        for h in range(HEADS):
            both_part[j, h * head : (h + 1) * head, :] = blend(sources, weights, total, h)
        for copy in fin_copies(j):
            copy.start()

    def turn(i, carry):
        j = i // 2
        odd = lax.rem(i, 2)
        group = owner_chip(j) * 2 + odd

        @pl.when(i == 1)
        def _():
            for s in range(late, chips):
                relay(s)

        @pl.when(odd != k)
        def _():
            await_col(group)

        q_now[...] = lax.dot_general(
            wq_t[...], fcol[group], (((1,), (1,)), ((), ())), preferred_element_type=f32
        ).astype(jnp.bfloat16)
        build_bias(group, table_ref, masks_ref, bias)

        @pl.when((i == cols - 2) & (i > 0))
        def _():
            merge(j - 1)

        attend_group(q_now, k_all, v_all, part.at[i], stat.at[i], bias, score)

        @pl.when(odd != k)
        def _():
            for copy in pair_copies(i, j):
                copy.start()

        @pl.when((odd == 0) & (i > 0) & (i < cols - 2))
        def _():
            merge(j - 1)

        return carry

    lax.fori_loop(0, cols, turn, 0)

    last = chips - 1
    mine = 2 * last + k
    for copy in pair_copies(0, last):
        copy.wait_recv()
    for j in range(last):
        for copy in fin_copies(j):
            copy.wait_recv()
    sources = [(part.at[mine], stat.at[mine]), (pair_part.at[last], pair_stat.at[last])]
    sources += [(fin_part.at[j], fin_stat.at[j]) for j in range(last)]
    _, weights, total = weigh(sources)
    for h in range(HEADS):
        out_ref[h * head : (h + 1) * head, :] = blend(sources, weights, total, h)

    for d in range(1, rows):
        to_row(d).wait_send()
    to_mate_left(0).wait_send()
    for s in range(chips):

        @pl.when(m >= s)
        def _():
            if s > 0:
                to_mate_left(s).wait_send()
            if s + 1 < chips:

                @pl.when(has_right)
                def _():
                    to_right(s).wait_send()

        @pl.when(m + s < chips)
        def _():
            if s > 0:
                to_mate_right(s).wait_send()
            if s + 1 < chips:

                @pl.when(has_left)
                def _():
                    to_left(s).wait_send()

    for j in range(chips):
        for copy in pair_copies(0, j):
            copy.wait_send()
    for j in range(last):
        for copy in fin_copies(j):
            copy.wait_send()


def fused(mesh_shape, table, masks, features, w_query, w_key, w_value):
    rows, cols = mesh_shape["row"], mesh_shape["col"]
    chips = cols // 2
    nodes, width = features.shape
    keys = rows * nodes
    head = width // HEADS
    bf16, f32 = jnp.bfloat16, jnp.float32
    whole = pl.BlockSpec(memory_space=pltpu.VMEM)
    dma = pltpu.SemaphoreType.DMA
    return pl.pallas_call(
        functools.partial(fused_kernel, rows, cols),
        out_shape=jax.ShapeDtypeStruct((width, nodes), bf16),
        in_specs=[pl.BlockSpec(memory_space=pltpu.SMEM)] + [whole] * 5,
        out_specs=whole,
        scratch_shapes=[
            pltpu.VMEM((rows, nodes, width), bf16),
            pltpu.VMEM((cols, nodes, width), bf16),
            pltpu.VMEM((width, width), bf16),
            pltpu.VMEM((width, width), bf16),
            pltpu.VMEM((keys, width), bf16),
            pltpu.VMEM((HEADS * (head + ONES), keys), bf16),
            pltpu.VMEM((width, nodes), bf16),
            pltpu.VMEM((cols, width, nodes), bf16),
            pltpu.VMEM((cols, 2 * HEADS, nodes), f32),
            pltpu.VMEM((chips, width, nodes), bf16),
            pltpu.VMEM((chips, 2 * HEADS, nodes), f32),
            pltpu.VMEM((chips, width, nodes), bf16),
            pltpu.VMEM((chips, 2 * HEADS, nodes), f32),
            pltpu.VMEM((chips, width, nodes), bf16),
            pltpu.VMEM((chips, 2 * HEADS, nodes), f32),
            pltpu.VMEM((keys, nodes), f32),
            pltpu.VMEM((2, keys, nodes), f32),
            dma((rows,)),
            dma((rows,)),
            dma((cols,)),
            dma((chips,)),
            dma((chips,)),
            dma((chips,)),
            dma((chips,)),
            dma((chips, 2)),
            dma((chips, 2)),
            dma((chips, 2)),
            dma((chips, 2)),
        ],
        compiler_params=pltpu.CompilerParams(
            collective_id=0, has_side_effects=True, vmem_limit_bytes=60 * 1024 * 1024
        ),
        name="fused",
    )(table, masks, features, w_query, w_key, w_value)


def entry_table(pairs, count, q_tiles, k_tiles):
    entries = pairs.shape[0]
    ids = lax.broadcasted_iota(jnp.int32, (q_tiles * k_tiles, entries), 1)
    cell = lax.broadcasted_iota(jnp.int32, (q_tiles * k_tiles, entries), 0)
    code = (pairs[:, 0] * k_tiles + pairs[:, 1])[None, :]
    return jnp.max(jnp.where((code == cell) & (ids < count), ids, -1), axis=1)


def body(mesh_shape, features, w_query, w_key, w_value, w_out, pairs, counts, masks):
    nodes = features.shape[0]
    rows, cols = mesh_shape["row"], mesh_shape["col"]
    table = entry_table(pairs[0, 0], counts[0, 0], cols * nodes // TILE, rows * nodes // TILE)
    words = masks[0, 0].transpose(0, 2, 1)
    attended = fused(mesh_shape, table, words, features, w_query, w_key, w_value)
    return lax.dot_general(
        attended, w_out, (((0,), (0,)), ((), ())), preferred_element_type=jnp.float32
    ).astype(jnp.bfloat16)


def solution(mesh):
    in_specs = (
        P(("row", "col"), None),
        P(),
        P(),
        P(),
        P(),
        P("row", "col", None, None),
        P("row", "col"),
        P("row", "col", None, None, None),
    )
    out_specs = P(("row", "col"), None)
    return jax.shard_map(
        functools.partial(body, dict(mesh.shape)), mesh=mesh, in_specs=in_specs, out_specs=out_specs, check_vma=False)
```

```python
import functools
import math

import jax
import jax.numpy as jnp
from jax import lax
from jax.experimental import pallas as pl
from jax.experimental.pallas import tpu as pltpu
from jax.sharding import PartitionSpec as P

HEADS = 8
TILE = 128
BLOCK = 512
ONES = 16
CHUNKS = 2


def build_bias(group, table_ref, masks_ref, bias_ref):
    keys, span = bias_ref.shape
    k_tiles = keys // TILE
    tiles = span // TILE
    shift = 31 - lax.broadcasted_iota(jnp.int32, (32, TILE), 0)
    for b in range(k_tiles):
        for t in range(tiles):
            entry = table_ref[(group * tiles + t) * k_tiles + b]
            words = masks_ref[jnp.maximum(entry, 0)] * jnp.where(entry >= 0, 1, 0)
            for j in range(TILE // 32):
                bits = jnp.broadcast_to(words[j : j + 1, :], (32, TILE)) << shift
                bias_ref[pl.ds(b * TILE + j * 32, 32), pl.ds(t * TILE, TILE)] = jnp.where(
                    bits < 0, 0.0, -jnp.inf
                )


def attend_group(queries, k_ref, v_ref, part_ref, stat_ref, bias_ref, score_ref):
    width, span = queries.shape
    keys = k_ref.shape[0]
    head = width // HEADS
    scale = 1.0 / math.sqrt(head)
    factor = scale * math.log2(math.e)
    v_rows = v_ref.shape[0] // HEADS
    step = min(BLOCK, keys)
    blocks = keys // step
    upper = lax.broadcasted_iota(jnp.int32, (2 * head, span), 0) < head

    def scores(h, block, top):
        pair = h // 2
        both = queries[pair * 2 * head : (pair + 1) * 2 * head, :]
        mine = jnp.where(upper == (h % 2 == 0), both, jnp.zeros_like(both))
        rows = slice(block * step, (block + 1) * step)
        raw = jnp.dot(
            k_ref[rows, pair * 2 * head : (pair + 1) * 2 * head],
            mine,
            preferred_element_type=jnp.float32,
        )
        raw = raw + bias_ref[rows, :]
        score_ref[h % 2, rows, :] = raw
        return jnp.maximum(top, jnp.max(raw.reshape(step // 8, 8, span), axis=0))

    def weighted(h, block, top, total):
        rows = slice(block * step, (block + 1) * step)
        prob = jnp.exp2((score_ref[h % 2, rows, :] - top) * factor).astype(jnp.bfloat16)
        term = jnp.dot(
            v_ref[h * v_rows : (h + 1) * v_rows, rows], prob, preferred_element_type=jnp.float32
        )
        return term if total is None else total + term

    def finish(h, top, total):
        peak = top * scale
        den = total[head : head + 1, :] + jnp.exp(-peak)
        part_ref[h * head : (h + 1) * head, :] = (total[:head, :] / den).astype(jnp.bfloat16)
        stat_ref[h : h + 1, :] = peak
        stat_ref[HEADS + h : HEADS + h + 1, :] = den

    zero = jnp.zeros((8, span), jnp.float32)
    tops = zero
    for block in range(blocks):
        tops = scores(0, block, tops)
    for h in range(HEADS):
        top = jnp.max(tops, axis=0, keepdims=True)
        total, tops = None, zero
        for block in range(blocks):
            if h + 1 < HEADS:
                tops = scores(h + 1, block, tops)
            total = weighted(h, block, top, total)
        finish(h, top, total)


MESH = pl.DeviceIdType.MESH


def fused_kernel(
    rows,
    cols,
    table_ref,
    masks_ref,
    features_ref,
    wq_ref,
    wk_ref,
    wv_ref,
    out_ref,
    frow,
    fcol,
    wq_t,
    wv_t,
    k_all,
    v_all,
    q_now,
    part,
    stat,
    pair_part,
    pair_stat,
    both_part,
    both_stat,
    fin_part,
    fin_stat,
    bias,
    score,
    row_send,
    row_recv,
    col_recv,
    right_send,
    left_send,
    share_left,
    share_right,
    pair_send,
    pair_recv,
    fin_send,
    fin_recv,
):
    nodes, width = features_ref.shape
    head = width // HEADS
    f32 = jnp.float32
    chips = cols // 2
    r, c = lax.axis_index("row"), lax.axis_index("col")
    m, k = c // 2, lax.rem(c, 2)
    mate = (r, m * 2 + 1 - k)

    half = chips // 2

    def at(chip):
        return (r, chip * 2 + k)

    def owner_chip(j):
        return lax.rem(m + jnp.where(j == 0, half, jnp.where(j < half, j, j + 1)), chips)

    def flip(place, b):
        return place + 1 - 2 * lax.rem(place, 2) if b else place

    def row_to(d):
        if rows % 2:
            return lax.rem(r + d, rows)
        return flip(lax.rem(r + d // 2 * 2, rows), d % 2)

    def row_from(d):
        if rows % 2:
            return lax.rem(r + rows - d, rows)
        return lax.rem(flip(r, d % 2) + rows - d // 2 * 2, rows)

    def send(src, dst, send_sem, recv_sem, device):
        return pltpu.make_async_remote_copy(
            src_ref=src,
            dst_ref=dst,
            send_sem=send_sem,
            recv_sem=recv_sem,
            device_id=device,
            device_id_type=MESH,
        )

    barrier = pltpu.get_barrier_semaphore()
    pl.semaphore_signal(barrier, inc=1, device_id=mate, device_id_type=MESH)
    for d in range(1, rows):
        peer = (lax.rem(r + d, rows), c)
        pl.semaphore_signal(barrier, inc=1, device_id=peer, device_id_type=MESH)
    for d in range(1, chips):
        peer = at(lax.rem(m + d, chips))
        pl.semaphore_signal(barrier, inc=1, device_id=peer, device_id_type=MESH)
    pl.semaphore_wait(barrier, 1 + rows - 1 + chips - 1)

    has_right, has_left = m + 1 < chips, m >= 1

    def hop(slot, own, piece, send_sem, device):
        size = nodes // CHUNKS
        span = pl.ds(piece * size, size)
        src = features_ref.at[span] if own else fcol.at[slot, span]
        return send(
            src, fcol.at[slot, span], send_sem.at[piece], col_recv.at[slot, piece], device
        )

    def to_right(s, piece):
        return hop((m - s) * 2 + k, s == 0, piece, right_send.at[s], at(m + 1))

    def to_left(s, piece):
        return hop((m + s) * 2 + k, s == 0, piece, left_send.at[s], at(m - 1))

    def to_mate_left(s, piece):
        return hop((m - s) * 2 + k, s == 0, piece, share_left.at[s], mate)

    def to_mate_right(s, piece):
        return hop((m + s) * 2 + k, s == 0, piece, share_right.at[s], mate)

    def to_row(d):
        return send(
            features_ref, frow.at[r], row_send.at[d], row_recv.at[r], (row_to(d), c)
        )

    def await_col(slot, piece):
        hop(slot, False, piece, right_send.at[0], mate).wait_recv()

    for piece in range(CHUNKS):

        @pl.when(has_right)
        def _():
            to_right(0, piece).start()

        @pl.when(has_left)
        def _():
            to_left(0, piece).start()

    for d in range(1, rows):
        to_row(d).start()
    for piece in range(CHUNKS):
        to_mate_left(0, piece).start()

    frow[r] = features_ref[...]
    fcol[c] = features_ref[...]
    wq_t[...] = wq_ref[...].T
    wv_t[...] = wv_ref[...].T
    for h in range(HEADS):
        v_all[h * (head + ONES) + head : (h + 1) * (head + ONES), :] = jnp.ones(
            (ONES, rows * nodes), jnp.bfloat16
        )

    def project_row(slot):
        block = frow[slot]
        lane = pl.ds(pl.multiple_of(slot * nodes, nodes), nodes)
        k_all[lane, :] = jnp.dot(block, wk_ref[...], preferred_element_type=f32).astype(
            jnp.bfloat16
        )
        value = lax.dot_general(
            wv_t[...], block, (((1,), (1,)), ((), ())), preferred_element_type=f32
        ).astype(jnp.bfloat16)
        for h in range(HEADS):
            v_all[h * (head + ONES) : h * (head + ONES) + head, lane] = value[
                h * head : (h + 1) * head, :
            ]

    project_row(r)

    def await_row(d):
        slot = row_from(d)
        send(frow.at[slot], frow.at[slot], row_send.at[0], row_recv.at[slot], mate).wait_recv()
        project_row(slot)

    def relay(s):
        for piece in range(CHUNKS):

            @pl.when(m >= s)
            def _():
                await_col((m - s) * 2 + k, piece)
                if s + 1 < chips:

                    @pl.when(has_right)
                    def _():
                        to_right(s, piece).start()

                to_mate_left(s, piece).start()

            @pl.when(m + s < chips)
            def _():
                await_col((m + s) * 2 + k, piece)
                if s + 1 < chips:

                    @pl.when(has_left)
                    def _():
                        to_left(s, piece).start()

                to_mate_right(s, piece).start()

    late = min(chips - half + 1, chips)
    for s in range(1, late):
        relay(s)
        if s == 1:
            for d in range(1, rows - 1):
                await_row(d)
    for d in range(rows - 1 if chips > 1 and late > 1 else 1, rows):
        await_row(d)

    def pair_copies(i, j):
        return (
            send(part.at[i], pair_part.at[j], pair_send.at[j, 0], pair_recv.at[j, 0], mate),
            send(stat.at[i], pair_stat.at[j], pair_send.at[j, 1], pair_recv.at[j, 1], mate),
        )

    def fin_copies(j):
        owner = at(owner_chip(j))
        return (
            send(both_part.at[j], fin_part.at[j], fin_send.at[j, 0], fin_recv.at[j, 0], owner),
            send(both_stat.at[j], fin_stat.at[j], fin_send.at[j, 1], fin_recv.at[j, 1], owner),
        )

    def weigh(sources):
        peaks = [ref[0:HEADS, :] for _, ref in sources]
        top = functools.reduce(jnp.maximum, peaks)
        weights = [
            jnp.exp(peak - top) * ref[HEADS : 2 * HEADS, :]
            for peak, (_, ref) in zip(peaks, sources)
        ]
        total = functools.reduce(jnp.add, weights)
        return top, weights, total

    def blend(sources, weights, total, h):
        rows_of = slice(h * head, (h + 1) * head)
        numer = functools.reduce(
            jnp.add,
            [
                ref[rows_of, :].astype(f32) * weight[h : h + 1, :]
                for weight, (ref, _) in zip(weights, sources)
            ],
        )
        return (numer / total[h : h + 1, :]).astype(jnp.bfloat16)

    def merge(j):
        for copy in pair_copies(0, j):
            copy.wait_recv()
        mine = 2 * j + k
        sources = [(part.at[mine], stat.at[mine]), (pair_part.at[j], pair_stat.at[j])]
        top, weights, total = weigh(sources)
        both_stat[j, 0:HEADS, :] = top
        both_stat[j, HEADS : 2 * HEADS, :] = total
        for h in range(HEADS):
            both_part[j, h * head : (h + 1) * head, :] = blend(sources, weights, total, h)
        for copy in fin_copies(j):
            copy.start()

    def turn(i, carry):
        j = i // 2
        odd = lax.rem(i, 2)
        group = owner_chip(j) * 2 + odd

        @pl.when(i == min(2, cols - 1))
        def _():
            for s in range(late, chips):
                relay(s)

        @pl.when(odd != k)
        def _():
            for piece in range(CHUNKS):
                await_col(group, piece)

        q_now[...] = lax.dot_general(
            wq_t[...], fcol[group], (((1,), (1,)), ((), ())), preferred_element_type=f32
        ).astype(jnp.bfloat16)
        build_bias(group, table_ref, masks_ref, bias)

        @pl.when((odd == 0) & (i > 0))
        def _():
            merge(j - 1)

        attend_group(q_now, k_all, v_all, part.at[i], stat.at[i], bias, score)

        @pl.when(odd != k)
        def _():
            for copy in pair_copies(i, j):
                copy.start()

        return carry

    lax.fori_loop(0, cols, turn, 0)

    last = chips - 1
    mine = 2 * last + k
    for copy in pair_copies(0, last):
        copy.wait_recv()
    for j in range(last):
        for copy in fin_copies(j):
            copy.wait_recv()
    sources = [(part.at[mine], stat.at[mine]), (pair_part.at[last], pair_stat.at[last])]
    sources += [(fin_part.at[j], fin_stat.at[j]) for j in range(last)]
    _, weights, total = weigh(sources)
    for h in range(HEADS):
        out_ref[h * head : (h + 1) * head, :] = blend(sources, weights, total, h)

    for d in range(1, rows):
        to_row(d).wait_send()
    for s in range(chips):
        for piece in range(CHUNKS):

            @pl.when(m >= s)
            def _():
                to_mate_left(s, piece).wait_send()
                if s + 1 < chips:

                    @pl.when(has_right)
                    def _():
                        to_right(s, piece).wait_send()

            @pl.when(m + s < chips)
            def _():
                if s > 0:
                    to_mate_right(s, piece).wait_send()
                if s + 1 < chips:

                    @pl.when(has_left)
                    def _():
                        to_left(s, piece).wait_send()

    for j in range(chips):
        for copy in pair_copies(0, j):
            copy.wait_send()
    for j in range(last):
        for copy in fin_copies(j):
            copy.wait_send()


def fused(mesh_shape, table, masks, features, w_query, w_key, w_value):
    rows, cols = mesh_shape["row"], mesh_shape["col"]
    chips = cols // 2
    nodes, width = features.shape
    keys = rows * nodes
    head = width // HEADS
    bf16, f32 = jnp.bfloat16, jnp.float32
    whole = pl.BlockSpec(memory_space=pltpu.VMEM)
    dma = pltpu.SemaphoreType.DMA
    return pl.pallas_call(
        functools.partial(fused_kernel, rows, cols),
        out_shape=jax.ShapeDtypeStruct((width, nodes), bf16),
        in_specs=[pl.BlockSpec(memory_space=pltpu.SMEM)] + [whole] * 5,
        out_specs=whole,
        scratch_shapes=[
            pltpu.VMEM((rows, nodes, width), bf16),
            pltpu.VMEM((cols, nodes, width), bf16),
            pltpu.VMEM((width, width), bf16),
            pltpu.VMEM((width, width), bf16),
            pltpu.VMEM((keys, width), bf16),
            pltpu.VMEM((HEADS * (head + ONES), keys), bf16),
            pltpu.VMEM((width, nodes), bf16),
            pltpu.VMEM((cols, width, nodes), bf16),
            pltpu.VMEM((cols, 2 * HEADS, nodes), f32),
            pltpu.VMEM((chips, width, nodes), bf16),
            pltpu.VMEM((chips, 2 * HEADS, nodes), f32),
            pltpu.VMEM((chips, width, nodes), bf16),
            pltpu.VMEM((chips, 2 * HEADS, nodes), f32),
            pltpu.VMEM((chips, width, nodes), bf16),
            pltpu.VMEM((chips, 2 * HEADS, nodes), f32),
            pltpu.VMEM((keys, nodes), f32),
            pltpu.VMEM((2, keys, nodes), f32),
            dma((rows,)),
            dma((rows,)),
            dma((cols, CHUNKS)),
            dma((chips, CHUNKS)),
            dma((chips, CHUNKS)),
            dma((chips, CHUNKS)),
            dma((chips, CHUNKS)),
            dma((chips, 2)),
            dma((chips, 2)),
            dma((chips, 2)),
            dma((chips, 2)),
        ],
        compiler_params=pltpu.CompilerParams(
            collective_id=0, has_side_effects=True, vmem_limit_bytes=60 * 1024 * 1024
        ),
        name="fused",
    )(table, masks, features, w_query, w_key, w_value)


def entry_table(pairs, count, q_tiles, k_tiles):
    entries = pairs.shape[0]
    ids = lax.broadcasted_iota(jnp.int32, (q_tiles * k_tiles, entries), 1)
    cell = lax.broadcasted_iota(jnp.int32, (q_tiles * k_tiles, entries), 0)
    code = (pairs[:, 0] * k_tiles + pairs[:, 1])[None, :]
    return jnp.max(jnp.where((code == cell) & (ids < count), ids, -1), axis=1)


def body(mesh_shape, features, w_query, w_key, w_value, w_out, pairs, counts, masks):
    nodes = features.shape[0]
    rows, cols = mesh_shape["row"], mesh_shape["col"]
    table = entry_table(pairs[0, 0], counts[0, 0], cols * nodes // TILE, rows * nodes // TILE)
    words = masks[0, 0].transpose(0, 2, 1)
    attended = fused(mesh_shape, table, words, features, w_query, w_key, w_value)
    return lax.dot_general(
        attended, w_out, (((0,), (0,)), ((), ())), preferred_element_type=jnp.float32
    ).astype(jnp.bfloat16)


def solution(mesh):
    in_specs = (
        P(("row", "col"), None),
        P(),
        P(),
        P(),
        P(),
        P("row", "col", None, None),
        P("row", "col"),
        P("row", "col", None, None, None),
    )
    out_specs = P(("row", "col"), None)
    return jax.shard_map(
        functools.partial(body, dict(mesh.shape)), mesh=mesh, in_specs=in_specs, out_specs=out_specs, check_vma=False)
```
